32 devices in a mesh: morton: 8 (over z, x), level: 4 (over y, core).
Axes of the slice: x: 2, y: 2, z: 4, core: 2. Of those that a mesh axis runs over, the one named last changes fastest.
Arguments:
- coarse_density: float32 [4096, 128], P('morton'), may hold values from 0.000125 to 0.12
- coarse_emission: float32 [4096, 128], P('morton'), may hold values from 0 to 4
- fine_density: float32 [16384, 128], P(('morton', 'level')), may hold values from 0.000125 to 0.12
- fine_emission: float32 [16384, 128], P(('morton', 'level')), may hold values from 0 to 4
- coarse_brick: int32 [32768], P(('morton', 'level')), may hold values from 0 to 15
- coarse_lane: int32 [32768], P(('morton', 'level')), may hold values from 0 to 1023
- coarse_entry: int32 [32768], P(('morton', 'level')), may hold values from 0 to 31, as said below
- coarse_count: int32 [32768], P(('morton', 'level')), may hold values from 0 to 32, as said below
- fine_owner: int32 [262144, 1], P(('morton', 'level')), may hold values from 0 to 31; in each aligned block of 8192 rows (0 to 8191, 8192 to 16383, ...) at most 512 rows name the same one
- fine_brick: int32 [262144], P(('morton', 'level')), may hold values from 0 to 1
- fine_lane: int32 [262144], P(('morton', 'level')), may hold values from 0 to 1023
- fine_entry: int32 [262144], P(('morton', 'level')), may hold values from 0 to 31, as said below
- fine_count: int32 [262144], P(('morton', 'level')), may hold values from 0 to 32, as said below
Outputs:
- image_color: float32 [8192], P(('morton', 'level'))
- transmittance: float32 [8192], P(('morton', 'level'))
The draws below stay inside these ranges and needn't reach their ends.
Inputs may be any that keep to these rules, and one draw needn't show every extreme that they name: `coarse_entry`: entry plus count is at most 32 for each segment. `coarse_count`: count 0 marks an empty segment. `fine_entry`: entry plus count is at most 32 for each segment. `fine_count`: count 0 marks a padded slot. `fine_owner`: among the fine segments of one device, at most 512 name one owner device, a bound that some block reaches.
All inputs are finite; a program needn't handle non-finite values.
Results may differ from the reference program's by a relative error of at most 0.0003.
Values sent between devices are 32-bit elements; how exact they have to be, the bound alone decides.
No kernel may reach another device: no remote copies, remote signals or barrier semaphores. Data moves between devices by JAX's collectives and lax.ppermute only.
A program may use at most 64 MiB of HBM per device.

```python
import math
import jax
import jax.numpy as jnp
import numpy as np
from jax import lax

BRICK = 32
BROWS = 256
FB = 2
CB = 16
GROUP_PIX = 1024
FSEG = 8
RCAP = 512
SLABSEG = 32768
SEGT = 262144
FINE = 64
N_MORTON = 8
N_LEVEL = 4


def entry_and_count(key, salt, total):
    inner = jax.random.fold_in(key, salt)
    first_key, second_key = jax.random.split(inner)
    entry_ids = jax.random.randint(first_key, (total,), 0, BRICK)
    count_ids = jax.random.randint(second_key, (total,), 0, BRICK - entry_ids + 1)
    return (entry_ids.astype(jnp.int32), count_ids.astype(jnp.int32))


def density_field(key, bricks):
    inner = jax.random.fold_in(key, 29)
    scale_key, cell_key = jax.random.split(inner)
    brick_scale = jnp.exp(jax.random.uniform(scale_key, (bricks, 1, 1), jnp.float32, math.log(0.0005), math.log(0.03)))
    cell_factor = jnp.exp(jax.random.uniform(cell_key, (bricks, BROWS, 128), jnp.float32, math.log(0.25), math.log(4.0)))
    return (brick_scale * cell_factor).reshape(bricks * BROWS, 128).astype(jnp.float32)


def draw_coarse_density(key, part):
    return density_field(key, CB)


def draw_fine_density(key, part):
    return density_field(key, FINE)


def draw_coarse_entry(key, part):
    return entry_and_count(key, 13, SLABSEG)[0]


def draw_coarse_count(key, part):
    return entry_and_count(key, 13, SLABSEG)[1]


def draw_fine_entry(key, part):
    return entry_and_count(key, 11, SEGT)[0]


def draw_fine_count(key, part):
    return entry_and_count(key, 11, SEGT)[1]


def touch_ends(drawn, stream_key, smallest, largest):
    place = [jax.random.randint(jax.random.fold_in(stream_key, axis), (), 0, length) for axis, length in enumerate(drawn.shape)]
    longest = drawn.shape.index(max(drawn.shape))
    beside = place[:longest] + [(place[longest] + 1) % drawn.shape[longest]] + place[longest + 1:]
    return drawn.at[tuple(place)].set(smallest).at[tuple(beside)].set(largest)


def steps_of(own_key, dims, shards, least, high):
    def one(axis_at, shards_of):
        heights = jax.random.uniform(jax.random.fold_in(jax.random.fold_in(own_key, 6), axis_at), (shards_of,), jnp.float32, least / len(shards), high / len(shards))
        return jnp.repeat(jnp.exp(heights), dims[axis_at] // shards_of).reshape((-1,) + (1,) * (len(dims) - axis_at - 1))

    factor_of = one(*shards[0])
    for cut in shards[1:]:
        factor_of = factor_of * one(*cut)
    return factor_of


def routed_block(stream_key, own, number, rows, amount, top, reach, lean):
    ranking = jax.random.permutation(stream_key, amount)
    crowded, common = shares(amount, rows * top, reach, lean, True), shares(amount, rows * top, reach, lean, False)
    places = jnp.arange(amount)

    def named(sizes, offset_by):
        used = int((sizes > 0).sum())
        fixed = max(1, used // 4)
        passed = fixed + (places - fixed + offset_by * (used - fixed)) % max(1, amount - fixed)
        return jnp.zeros((amount,), jnp.int32).at[ranking[jnp.where(places < fixed, places, passed)]].set(jnp.asarray(sizes, jnp.int32))

    sizes = jnp.where(number % 4 == 0, named(crowded, number // 4), named(common, number - number // 4 - 1))
    mixed = jax.random.permutation(jax.random.fold_in(own, 3), amount)
    giver, taker = mixed[0:amount // 2 * 2:2], mixed[1:amount // 2 * 2:2]
    slack = jnp.minimum(sizes[giver] - 1, reach - sizes[taker]) // 2
    slack = jnp.where((giver == ranking[0]) | (taker == ranking[0]) | (sizes[taker] == 0), 0, jnp.maximum(slack, 0))
    passed = jax.random.randint(jax.random.fold_in(own, 4), (amount // 2,), 0, 1 << 20) % (slack + 1)
    sizes = sizes.at[giver].add(-passed).at[taker].add(passed)
    items = jnp.searchsorted(jnp.cumsum(sizes), jnp.arange(rows * top), side="right").astype(jnp.int32)
    listing = items.reshape(top, rows).T
    listing = listing[jax.random.permutation(jax.random.fold_in(own, 1), rows)]
    offset_by = jax.random.randint(jax.random.fold_in(own, 2), (rows, 1), 0, top)
    return jnp.take_along_axis(listing, (jnp.arange(top)[None, :] + offset_by) % top, axis=1)


def shares(amount, total, bound, skew, full):
    loads = [(1 << 20) // math.isqrt(standing ** skew) + 1 for standing in range(1, amount + 1)]
    largest = bound if full else min(bound, max(-(-total // amount), total * loads[0] // sum(loads)))
    least = 1 if total - largest >= amount - 1 else 0
    counts, rest = [largest] + [least] * (amount - 1), total - largest - least * (amount - 1)
    while rest > 0:
        free = [i for i in range(1, amount) if counts[i] < largest] or [i for i in range(1, amount) if counts[i] < bound]
        whole, left = sum([loads[i] for i in free]), rest
        for i in free:
            addition = min(bound - counts[i], max(1, left * loads[i] // whole), rest)
            counts[i] = counts[i] + addition
            rest = rest - addition
    return np.array(counts)


def setup_inputs(seed: int = 0) -> dict:
    key_of = jax.random.split(jax.random.key(seed), 14)
    coarse_density = draw_coarse_density(jax.random.fold_in(key_of[13], 71), 0)
    coarse_emission = jnp.clip(4.0 * jax.random.uniform(key_of[1], (CB * BROWS, 128), jnp.float32) ** steps_of(key_of[1], (CB * BROWS, 128), ((0, 8),), -0.2, 0.2), 0.0, 4.0)
    fine_density = draw_fine_density(jax.random.fold_in(key_of[13], 71), 0)
    fine_emission = jnp.clip(4.0 * jax.random.uniform(key_of[3], (FINE * BROWS, 128), jnp.float32) ** steps_of(key_of[3], (FINE * BROWS, 128), ((0, 32),), -0.2, 0.2), 0.0, 4.0)
    coarse_brick = touch_ends(jax.random.randint(key_of[4], (SLABSEG,), 0, CB), jax.random.fold_in(key_of[4], 1), 0, CB - 1).astype(jnp.int32)
    coarse_lane = touch_ends(jax.random.randint(key_of[5], (SLABSEG,), 0, BRICK * BRICK), jax.random.fold_in(key_of[5], 1), 0, (BRICK * BRICK) - 1).astype(jnp.int32)
    coarse_entry = draw_coarse_entry(jax.random.fold_in(key_of[13], 71), 0)
    coarse_count = draw_coarse_count(jax.random.fold_in(key_of[13], 71), 0)
    fine_owner_keys = jax.random.split(jax.random.fold_in(key_of[8], 1), SEGT // (GROUP_PIX * FSEG))
    fine_owner_turns = jax.random.permutation(jax.random.fold_in(key_of[8], 3), SEGT // (GROUP_PIX * FSEG))
    fine_owner = jax.vmap(lambda own, number: routed_block(jax.random.fold_in(key_of[8], 2), own, number, GROUP_PIX * FSEG, N_MORTON * N_LEVEL, 1, RCAP, 2))(fine_owner_keys, fine_owner_turns).reshape((SEGT, 1))
    fine_brick = touch_ends(jax.random.randint(key_of[9], (SEGT,), 0, FB), jax.random.fold_in(key_of[9], 1), 0, FB - 1).astype(jnp.int32)
    fine_lane = touch_ends(jax.random.randint(key_of[10], (SEGT,), 0, BRICK * BRICK), jax.random.fold_in(key_of[10], 1), 0, (BRICK * BRICK) - 1).astype(jnp.int32)
    fine_entry = draw_fine_entry(jax.random.fold_in(key_of[13], 71), 0)
    fine_count = draw_fine_count(jax.random.fold_in(key_of[13], 71), 0)
    return {"coarse_density": coarse_density, "coarse_emission": coarse_emission, "fine_density": fine_density, "fine_emission": fine_emission, "coarse_brick": coarse_brick, "coarse_lane": coarse_lane, "coarse_entry": coarse_entry, "coarse_count": coarse_count, "fine_owner": fine_owner, "fine_brick": fine_brick, "fine_lane": fine_lane, "fine_entry": fine_entry, "fine_count": fine_count}


def march(density_rows, emission_rows, lane_ids, entry_ids, count_ids):
    per_row = 128 // BRICK
    chosen = ((lane_ids % per_row)[:, None] == lax.broadcasted_iota(jnp.int32, (1, per_row), 1))[:, :, None]
    nothing = jnp.float32(0.0)
    dens_lane = jnp.sum(jnp.where(chosen, density_rows.reshape(-1, per_row, BRICK), nothing), axis=1).T
    emis_lane = jnp.sum(jnp.where(chosen, emission_rows.reshape(-1, per_row, BRICK), nothing), axis=1).T
    step_ids = lax.broadcasted_iota(jnp.int32, (BRICK, 1), 0)
    inside = (step_ids >= entry_ids[None, :]) & (step_ids < (entry_ids + count_ids)[None, :])
    optical = jnp.where(inside, dens_lane, nothing)
    before = jnp.cumsum(optical, axis=0) - optical
    opacity = 1.0 - jnp.exp(-optical)
    colors = jnp.sum(jnp.exp(-before) * opacity * emis_lane, axis=0)
    return colors, jnp.sum(optical, axis=0)


def sample_table(dens_table, emis_table, brick_ids, lane_ids, entry_ids, count_ids):
    row_index = brick_ids * BROWS + lane_ids // (128 // BRICK)
    return march(dens_table[row_index], emis_table[row_index], lane_ids, entry_ids, count_ids)


def reference(coarse_density, coarse_emission, fine_density, fine_emission, coarse_brick, coarse_lane, coarse_entry, coarse_count, fine_owner, fine_brick, fine_lane, fine_entry, fine_count):
    groups = N_MORTON * N_LEVEL
    owner = fine_owner[:, 0]

    def one_slab(inputs):
        c_brick, c_lane, c_entry, c_count, f_owner, f_brick, f_lane, f_entry, f_count = inputs
        coarse_color, coarse_depth = sample_table(coarse_density, coarse_emission, c_brick, c_lane, c_entry, c_count)
        global_brick = f_owner * FB + f_brick
        seg_color, seg_depth = sample_table(fine_density, fine_emission, global_brick, f_lane, f_entry, f_count)
        seg_color = seg_color.reshape(GROUP_PIX, FSEG)
        seg_depth = seg_depth.reshape(GROUP_PIX, FSEG)
        earlier = jnp.cumsum(seg_depth, axis=1) - seg_depth
        slab_color = coarse_color + jnp.exp(-coarse_depth) * jnp.sum(jnp.exp(-earlier) * seg_color, axis=1)
        slab_depth = coarse_depth + jnp.sum(seg_depth, axis=1)
        return slab_color, slab_depth

    inputs = (coarse_brick.reshape(groups, GROUP_PIX), coarse_lane.reshape(groups, GROUP_PIX), coarse_entry.reshape(groups, GROUP_PIX), coarse_count.reshape(groups, GROUP_PIX), owner.reshape(groups, GROUP_PIX * FSEG), fine_brick.reshape(groups, GROUP_PIX * FSEG), fine_lane.reshape(groups, GROUP_PIX * FSEG), fine_entry.reshape(groups, GROUP_PIX * FSEG), fine_count.reshape(groups, GROUP_PIX * FSEG))
    slab_color, slab_depth = lax.map(one_slab, inputs)
    slab_color = slab_color.reshape(N_MORTON, N_LEVEL, GROUP_PIX)
    slab_depth = slab_depth.reshape(N_MORTON, N_LEVEL, GROUP_PIX)
    earlier = jnp.cumsum(slab_depth, axis=1) - slab_depth
    image_color = jnp.sum(jnp.exp(-earlier) * slab_color, axis=1).reshape(N_MORTON * GROUP_PIX)
    transmittance = jnp.exp(-jnp.sum(slab_depth, axis=1)).reshape(N_MORTON * GROUP_PIX)
    return image_color, transmittance
```

```python
import functools

import jax
import jax.numpy as jnp
from jax import lax
from jax.experimental import pallas as pl
from jax.experimental.pallas import tpu as pltpu
from jax.sharding import PartitionSpec as P

BRICK = 32
PER_ROW = 128 // BRICK
AXES = ("morton", "level")
F32 = jnp.float32
BF16 = jnp.bfloat16


def split3(x):
    hi = x.astype(BF16)
    rest = x - hi.astype(F32)
    mid = rest.astype(BF16)
    lo = (rest - mid.astype(F32)).astype(BF16)
    return hi, mid, lo


def split2(x):
    hi = x.astype(BF16)
    return hi, (x - hi.astype(F32)).astype(BF16)


def flag(cond):
    return jnp.where(cond, F32(1.0), F32(0.0)).astype(BF16)


def iota(shape, axis):
    return lax.broadcasted_iota(jnp.int32, shape, axis)


def line(ref, start, rows):
    return jnp.concatenate([ref[start + j : start + j + 1, :] for j in range(rows)], axis=1)


def nt_dot(a, b):
    return lax.dot_general(a, b, (((1,), (1,)), ((), ())), preferred_element_type=F32)


def route_kernel(owner, brick, lane, entry, count, cbrick, clane, centry, ccount, msg, ranks, *, n_dev, n_level, cap, quarter):
    rows = owner.shape[0]
    per = 4
    width = per * 128
    upper = flag(iota((width, width), 0) < iota((width, width), 1))
    t_ids = iota((n_dev, width), 0)
    r_ids = iota((cap, width), 0)
    offsets = jnp.zeros((n_dev, 1), F32)
    acc = jnp.zeros((3 * n_dev, cap), F32)
    for c in range(rows // per):
        own = line(owner, c * per, per)
        hit = own == t_ids
        hot = jnp.where(hit, F32(1.0), F32(0.0))
        before = jnp.dot(hot.astype(BF16), upper, preferred_element_type=F32)
        rank = jnp.sum(hot * (before + offsets), axis=0, keepdims=True)
        offsets = offsets + before[:, width - 1 :] + hot[:, width - 1 :]
        rank_int = rank.astype(jnp.int32)
        ranks[c : c + 1, :] = rank_int
        cell = line(brick, c * per, per) * (BRICK * BRICK) + line(lane, c * per, per)
        code = (cell * BRICK + line(entry, c * per, per)) * 64 + line(count, c * per, per)
        parts = [(code & 255), ((code >> 8) & 255), (code >> 16)]
        left = jnp.concatenate(
            [jnp.where(hit, part.astype(F32), F32(0.0)).astype(BF16) for part in parts], axis=0
        )
        acc = acc + nt_dot(left, flag(rank_int == r_ids))
    fine = acc[:n_dev] + acc[n_dev : 2 * n_dev] * F32(256.0) + acc[2 * n_dev :] * F32(65536.0)
    msg[:, quarter:] = fine.astype(jnp.int32)
    level_of = iota((n_dev, quarter), 0) % n_level
    crows = quarter // 128
    out = jnp.zeros((n_dev, quarter), jnp.int32)
    for q in range(n_level):
        cell = line(cbrick, q * crows, crows) * (BRICK * BRICK) + line(clane, q * crows, crows)
        code = (cell * BRICK + line(centry, q * crows, crows)) * 64 + line(ccount, q * crows, crows)
        out = jnp.where(level_of == q, code, out)
    msg[:, :quarter] = out


def march_block(table, code, base):
    rows = table.shape[2]
    width = code.shape[1]
    row = (code >> 13) - base
    hot = flag(row == iota((rows, width), 0))
    both = jnp.dot(table[0], hot, preferred_element_type=F32) + jnp.dot(
        table[1], hot, preferred_element_type=F32
    )
    which = (code >> 11) & (PER_ROW - 1)
    entry = (code >> 6) & (BRICK - 1)
    end = entry + (code & 63)

    def pick(start):
        out = both[start : start + BRICK]
        for j in range(1, PER_ROW):
            out = jnp.where(which == j, both[start + j * BRICK : start + (j + 1) * BRICK], out)
        return out

    dens, emis = pick(0), pick(128)
    step = iota((BRICK, width), 0)
    optical = jnp.where((step >= entry) & (step < end), dens, F32(0.0))
    run = jnp.zeros((1, width), F32)
    color = jnp.zeros((8, width), F32)
    sub = iota((8, width), 0)
    for g in range(BRICK // 8):
        mine = optical[g * 8 : g * 8 + 8]
        scan = mine
        for shift in (1, 2, 4):
            scan = scan + jnp.where(sub >= shift, pltpu.roll(scan, shift, 0), F32(0.0))
        before = (scan - mine) + run
        color = color + jnp.exp(-before) * (1.0 - jnp.exp(-mine)) * emis[g * 8 : g * 8 + 8]
        run = run + scan[7:8]
    return jnp.sum(color, axis=0, keepdims=True), run


def load_table(dens, emis, table):
    dens_hi, dens_lo = split2(dens[...].T)
    emis_hi, emis_lo = split2(emis[...].T)
    table[0, :128, :] = dens_hi
    table[0, 128:, :] = emis_hi
    table[1, :128, :] = dens_lo
    table[1, 128:, :] = emis_lo


def march_kernel(base, msg, fdens, femis, cdens, cemis, out, ftable, ctable, *, quarter):
    n_dev = msg.shape[0]
    load_table(fdens, femis, ftable)
    load_table(cdens, cemis, ctable)
    start = base[0]

    def body(s, carry):
        code = msg[pl.ds(s, 1), :]
        near = march_block(ctable, code[:, :quarter], start)
        far = march_block(ftable, code[:, quarter:], 0)
        out[pl.ds(s, 1), :] = jnp.concatenate([near[0], far[0], near[1], far[1]], axis=1)
        return carry

    lax.fori_loop(0, n_dev, body, 0)


def blend_kernel(back, owner, ranks, out, color_ref, depth_ref, *, n_level, quarter, per_pixel):
    n_dev, width = back.shape[0], back.shape[1] // 2
    cap = width - quarter
    rows = owner.shape[0]
    per = 4
    chunk = per * 128
    line_len = quarter * per_pixel
    stacked = jnp.concatenate(split3(back[:, quarter:width]) + split3(back[:, width + quarter :]), axis=0)
    t_ids = iota((n_dev, chunk), 0)
    r_ids = iota((cap, chunk), 0)
    for c in range(rows // per):
        hit = line(owner, c * per, per) == t_ids
        hot = flag(ranks[c : c + 1, :] == r_ids)
        got = jnp.dot(stacked, hot, preferred_element_type=F32)
        picked = [
            jnp.sum(
                jnp.where(
                    hit,
                    got[k * n_dev : (k + 1) * n_dev]
                    + got[(k + 1) * n_dev : (k + 2) * n_dev]
                    + got[(k + 2) * n_dev : (k + 3) * n_dev],
                    F32(0.0),
                ),
                axis=0,
                keepdims=True,
            )
            for k in (0, 3)
        ]
        at, off = divmod(c * chunk, line_len)
        color_ref[at : at + 1, off : off + chunk] = picked[0]
        depth_ref[at : at + 1, off : off + chunk] = picked[1]
    depth = depth_ref[...]
    slot = iota((n_level, line_len), 1) % per_pixel
    scan = depth
    shift = 1
    while shift < per_pixel:
        scan = scan + jnp.where(slot >= shift, pltpu.roll(scan, shift, 1), F32(0.0))
        shift *= 2
    seen = jnp.exp(-(scan - depth)) * color_ref[...]
    gather = flag(iota((line_len, quarter), 0) // per_pixel == iota((line_len, quarter), 1))
    sums = jnp.dot(
        jnp.concatenate([x.astype(F32) for x in split3(seen) + split3(depth)], axis=0).astype(BF16),
        gather,
        preferred_element_type=F32,
    )
    part = [sums[k * n_level : (k + 1) * n_level] for k in range(6)]
    fine_color, fine_depth = part[0] + part[1] + part[2], part[3] + part[4] + part[5]

    def coarse(start):
        block = back[:, start : start + quarter]
        total = block[:n_level]
        for m in range(1, n_dev // n_level):
            total = total + block[m * n_level : (m + 1) * n_level]
        return total

    coarse_color, coarse_depth = coarse(0), coarse(width)
    out[:, :quarter] = coarse_color + jnp.exp(-coarse_depth) * fine_color
    out[:, quarter:] = coarse_depth + fine_depth


def shards(
    coarse_density,
    coarse_emission,
    fine_density,
    fine_emission,
    coarse_brick,
    coarse_lane,
    coarse_entry,
    coarse_count,
    fine_owner,
    fine_brick,
    fine_lane,
    fine_entry,
    fine_count,
):
    n_morton = lax.axis_size("morton")
    n_level = lax.axis_size("level")
    n_dev = n_morton * n_level
    segments = fine_brick.shape[0]
    pixels = coarse_brick.shape[0]
    quarter = pixels // n_level
    cap = -(-(2 * segments // n_dev) // 128) * 128
    width = quarter + cap
    owner = fine_owner.reshape(-1, 128)
    fine = [x.reshape(-1, 128) for x in (fine_brick, fine_lane, fine_entry, fine_count)]
    coarse = [x.reshape(-1, 128) for x in (coarse_brick, coarse_lane, coarse_entry, coarse_count)]
    msg, ranks = pl.pallas_call(
        functools.partial(route_kernel, n_dev=n_dev, n_level=n_level, cap=cap, quarter=quarter),
        out_shape=(
            jax.ShapeDtypeStruct((n_dev, width), jnp.int32),
            jax.ShapeDtypeStruct((segments // 512, 512), jnp.int32),
        ),
        name="route",
    )(owner, *fine, *coarse)
    msg = lax.all_to_all(msg, AXES, split_axis=0, concat_axis=0, tiled=True)
    base = (lax.axis_index("morton") * coarse_density.shape[0]).reshape(1)
    vmem = pl.BlockSpec(memory_space=pltpu.VMEM)
    served = pl.pallas_call(
        functools.partial(march_kernel, quarter=quarter),
        out_shape=jax.ShapeDtypeStruct((n_dev, 2 * width), F32),
        in_specs=[pl.BlockSpec(memory_space=pltpu.SMEM)] + [vmem] * 5,
        out_specs=vmem,
        scratch_shapes=[
            pltpu.VMEM((2, 256, fine_density.shape[0]), BF16),
            pltpu.VMEM((2, 256, coarse_density.shape[0]), BF16),
        ],
        name="march",
    )(base, msg, fine_density, fine_emission, coarse_density, coarse_emission)
    back = lax.all_to_all(served, AXES, split_axis=0, concat_axis=0, tiled=True)
    per_pixel = segments // pixels
    slab = pl.pallas_call(
        functools.partial(blend_kernel, n_level=n_level, quarter=quarter, per_pixel=per_pixel),
        out_shape=jax.ShapeDtypeStruct((n_level, 2 * quarter), F32),
        scratch_shapes=[pltpu.VMEM((n_level, quarter * per_pixel), F32)] * 2,
        name="blend",
    )(back, owner, ranks)
    slabs = lax.all_to_all(slab, "level", split_axis=0, concat_axis=0, tiled=True)
    part_color, part_depth = slabs[:, :quarter], slabs[:, quarter:]
    in_front = jnp.cumsum(part_depth, axis=0) - part_depth
    image_color = jnp.sum(jnp.exp(-in_front) * part_color, axis=0)
    transmittance = jnp.exp(-jnp.sum(part_depth, axis=0))
    return (image_color, transmittance)


def solution(mesh):
    split = P(AXES)
    rows = P(AXES, None)
    return jax.shard_map(
        shards,
        mesh=mesh,
        in_specs=(P("morton", None), P("morton", None), rows, rows)
        + (split,) * 4
        + (rows,)
        + (split,) * 4,
        out_specs=(split, split),
        check_vma=False,
    )
```

```python
import functools

import jax
import jax.numpy as jnp
from jax import lax
from jax.experimental import pallas as pl
from jax.experimental.pallas import tpu as pltpu
from jax.sharding import PartitionSpec as P

BRICK = 32
PER_ROW = 128 // BRICK
UNROLL = 8
AXES = ("morton", "level")
F32 = jnp.float32
BF16 = jnp.bfloat16


def split3(x):
    hi = x.astype(BF16)
    rest = x - hi.astype(F32)
    mid = rest.astype(BF16)
    lo = (rest - mid.astype(F32)).astype(BF16)
    return hi, mid, lo


def split2(x):
    hi = x.astype(BF16)
    return hi, (x - hi.astype(F32)).astype(BF16)


def flag(cond):
    return jnp.where(cond, F32(1.0), F32(0.0)).astype(BF16)


def iota(shape, axis):
    return lax.broadcasted_iota(jnp.int32, shape, axis)


def line(ref, start, rows):
    return jnp.concatenate([ref[start + j : start + j + 1, :] for j in range(rows)], axis=1)


def nt_dot(a, b):
    return lax.dot_general(a, b, (((1,), (1,)), ((), ())), preferred_element_type=F32)


def route_kernel(owner, brick, lane, entry, count, cbrick, clane, centry, ccount, msg, ranks, *, n_dev, n_level, cap, quarter):
    rows = owner.shape[0]
    per = 4
    width = per * 128
    upper = flag(iota((width, width), 0) < iota((width, width), 1))
    t_ids = iota((n_dev, width), 0)
    r_ids = iota((cap, width), 0)
    offsets = jnp.zeros((n_dev, 1), F32)
    acc = jnp.zeros((3 * n_dev, cap), F32)
    for c in range(rows // per):
        own = line(owner, c * per, per)
        hit = own == t_ids
        hot = jnp.where(hit, F32(1.0), F32(0.0))
        before = jnp.dot(hot.astype(BF16), upper, preferred_element_type=F32)
        rank = jnp.sum(hot * (before + offsets), axis=0, keepdims=True)
        offsets = offsets + before[:, width - 1 :] + hot[:, width - 1 :]
        rank_int = rank.astype(jnp.int32)
        ranks[c : c + 1, :] = rank_int
        cell = line(brick, c * per, per) * (BRICK * BRICK) + line(lane, c * per, per)
        code = (cell * BRICK + line(entry, c * per, per)) * 64 + line(count, c * per, per)
        parts = [(code & 255), ((code >> 8) & 255), (code >> 16)]
        left = jnp.concatenate(
            [jnp.where(hit, part.astype(F32), F32(0.0)).astype(BF16) for part in parts], axis=0
        )
        acc = acc + nt_dot(left, flag(rank_int == r_ids))
    fine = acc[:n_dev] + acc[n_dev : 2 * n_dev] * F32(256.0) + acc[2 * n_dev :] * F32(65536.0)
    fine = fine.astype(jnp.int32)
    level_of = iota((n_dev, quarter), 0) % n_level
    crows = quarter // 128
    out = jnp.zeros((n_dev, quarter), jnp.int32)
    for q in range(n_level):
        cell = line(cbrick, q * crows, crows) * (BRICK * BRICK) + line(clane, q * crows, crows)
        code = (cell * BRICK + line(centry, q * crows, crows)) * 64 + line(ccount, q * crows, crows)
        out = jnp.where(level_of == q, code, out)
    msg[:, 0, :quarter] = out
    msg[:, 0, quarter:] = fine


def march_block(table, code, base):
    rows = table.shape[1]
    width = code.shape[1]
    row = (code >> 13) - base
    seg = min(rows, 256)
    lane_row = iota((seg, width), 0).astype(F32).astype(BF16)
    parts = []
    for h in range(rows // seg):
        mine = row - h * seg
        mine = jnp.where((mine >= 0) & (mine < seg), mine, -1).astype(F32).astype(BF16)
        parts.append(jnp.where(lane_row == mine, BF16(1.0), BF16(0.0)))
    hot = jnp.concatenate(parts, axis=0)
    pieces = jnp.dot(table[...], hot, preferred_element_type=F32)
    both = pieces[:256] + pieces[256:]
    which = (code >> 11) & (PER_ROW - 1)
    entry = (code >> 6) & (BRICK - 1)
    end = entry + (code & 63)

    def pick(start):
        out = both[start : start + BRICK]
        for j in range(1, PER_ROW):
            out = jnp.where(which == j, both[start + j * BRICK : start + (j + 1) * BRICK], out)
        return out

    dens, emis = pick(0), pick(128)
    step = iota((BRICK, width), 0)
    optical = jnp.where((step >= entry) & (step < end), dens, F32(0.0))
    run = jnp.zeros((1, width), F32)
    color = jnp.zeros((8, width), F32)
    sub = iota((8, width), 0)
    for g in range(BRICK // 8):
        mine = optical[g * 8 : g * 8 + 8]
        scan = mine
        for shift in (1, 2, 4):
            scan = scan + jnp.where(sub >= shift, pltpu.roll(scan, shift, 0), F32(0.0))
        before = (scan - mine) + run
        color = color + jnp.exp(-before) * (1.0 - jnp.exp(-mine)) * emis[g * 8 : g * 8 + 8]
        run = run + scan[7:8]
    return jnp.sum(color, axis=0, keepdims=True), run


def load_table(dens, emis, table):
    dens_hi, dens_lo = split2(dens[...].T)
    emis_hi, emis_lo = split2(emis[...].T)
    table[:128, :] = dens_hi
    table[128:256, :] = emis_hi
    table[256:384, :] = dens_lo
    table[384:, :] = emis_lo


def march_kernel(base, msg, fdens, femis, cdens, cemis, out, ftable, ctable, *, quarter):
    n_dev = msg.shape[0]
    load_table(fdens, femis, ftable)
    load_table(cdens, cemis, ctable)
    start = base[0]

    def body(s, carry):
        code = msg[s]
        near = march_block(ctable, code[:, :quarter], start)
        far = march_block(ftable, code[:, quarter:], 0)
        out[s] = jnp.concatenate([near[0], far[0], near[1], far[1]], axis=1)
        return carry

    lax.fori_loop(0, n_dev, body, 0, unroll=UNROLL)


def blend_kernel(back, owner, ranks, out, color_ref, depth_ref, *, n_level, quarter, per_pixel):
    n_dev, width = back.shape[0], back.shape[2] // 2

    def cut(start, end):
        return back[:, 0, start:end]

    cap = width - quarter
    rows = owner.shape[0]
    per = 4
    chunk = per * 128
    line_len = quarter * per_pixel
    stacked = jnp.concatenate(split3(cut(quarter, width)) + split3(cut(width + quarter, 2 * width)), axis=0)
    t_ids = iota((n_dev, chunk), 0)
    r_ids = iota((cap, chunk), 0)
    for c in range(rows // per):
        hit = line(owner, c * per, per) == t_ids
        hot = flag(ranks[c : c + 1, :] == r_ids)
        got = jnp.dot(stacked, hot, preferred_element_type=F32)
        picked = [
            jnp.sum(
                jnp.where(
                    hit,
                    got[k * n_dev : (k + 1) * n_dev]
                    + got[(k + 1) * n_dev : (k + 2) * n_dev]
                    + got[(k + 2) * n_dev : (k + 3) * n_dev],
                    F32(0.0),
                ),
                axis=0,
                keepdims=True,
            )
            for k in (0, 3)
        ]
        at, off = divmod(c * chunk, line_len)
        color_ref[at : at + 1, off : off + chunk] = picked[0]
        depth_ref[at : at + 1, off : off + chunk] = picked[1]
    depth = depth_ref[...]
    slot = iota((n_level, line_len), 1) % per_pixel
    scan = depth
    shift = 1
    while shift < per_pixel:
        scan = scan + jnp.where(slot >= shift, pltpu.roll(scan, shift, 1), F32(0.0))
        shift *= 2
    seen = jnp.exp(-(scan - depth)) * color_ref[...]
    gather = flag(iota((line_len, quarter), 0) // per_pixel == iota((line_len, quarter), 1))
    sums = jnp.dot(
        jnp.concatenate([x.astype(F32) for x in split3(seen) + split3(depth)], axis=0).astype(BF16),
        gather,
        preferred_element_type=F32,
    )
    part = [sums[k * n_level : (k + 1) * n_level] for k in range(6)]
    fine_color, fine_depth = part[0] + part[1] + part[2], part[3] + part[4] + part[5]

    def coarse(start):
        block = cut(start, start + quarter)
        total = block[:n_level]
        for m in range(1, n_dev // n_level):
            total = total + block[m * n_level : (m + 1) * n_level]
        return total

    coarse_color, coarse_depth = coarse(0), coarse(width)
    out[:, 0, :quarter] = coarse_color + jnp.exp(-coarse_depth) * fine_color
    out[:, 0, quarter:] = coarse_depth + fine_depth


def finish_kernel(slabs, color_ref, through_ref):
    quarter = slabs.shape[2] // 2
    color = jnp.zeros((1, quarter), F32)
    depth = jnp.zeros((1, quarter), F32)
    for s in range(slabs.shape[0]):
        part = slabs[s]
        color = color + jnp.exp(-depth) * part[:, :quarter]
        depth = depth + part[:, quarter:]
    color_ref[...] = color
    through_ref[...] = jnp.exp(-depth)


def shards(
    coarse_density,
    coarse_emission,
    fine_density,
    fine_emission,
    coarse_brick,
    coarse_lane,
    coarse_entry,
    coarse_count,
    fine_owner,
    fine_brick,
    fine_lane,
    fine_entry,
    fine_count,
):
    n_morton = lax.axis_size("morton")
    n_level = lax.axis_size("level")
    n_dev = n_morton * n_level
    segments = fine_brick.shape[0]
    pixels = coarse_brick.shape[0]
    quarter = pixels // n_level
    cap = -(-(2 * segments // n_dev) // 128) * 128
    width = quarter + cap
    owner = fine_owner.reshape(-1, 128)
    fine = [x.reshape(-1, 128) for x in (fine_brick, fine_lane, fine_entry, fine_count)]
    coarse = [x.reshape(-1, 128) for x in (coarse_brick, coarse_lane, coarse_entry, coarse_count)]
    msg, ranks = pl.pallas_call(
        functools.partial(route_kernel, n_dev=n_dev, n_level=n_level, cap=cap, quarter=quarter),
        out_shape=(
            pltpu.VMEM((n_dev, 1, width), jnp.int32),
            jax.ShapeDtypeStruct((segments // 512, 512), jnp.int32),
        ),
        name="route",
    )(owner, *fine, *coarse)
    msg = lax.all_to_all(msg, AXES, split_axis=0, concat_axis=0, tiled=True)
    msg = pltpu.with_memory_space_constraint(msg, pltpu.VMEM)
    base = (lax.axis_index("morton") * coarse_density.shape[0]).reshape(1)
    vmem = pl.BlockSpec(memory_space=pltpu.VMEM)
    served = pl.pallas_call(
        functools.partial(march_kernel, quarter=quarter),
        out_shape=pltpu.VMEM((n_dev, 1, 2 * width), F32),
        in_specs=[pl.BlockSpec(memory_space=pltpu.SMEM)] + [vmem] * 5,
        out_specs=vmem,
        scratch_shapes=[
            pltpu.VMEM((512, fine_density.shape[0]), BF16),
            pltpu.VMEM((512, coarse_density.shape[0]), BF16),
        ],
        name="march",
    )(base, msg, fine_density, fine_emission, coarse_density, coarse_emission)
    back = lax.all_to_all(served, AXES, split_axis=0, concat_axis=0, tiled=True)
    back = pltpu.with_memory_space_constraint(back, pltpu.VMEM)
    per_pixel = segments // pixels
    slab = pl.pallas_call(
        functools.partial(blend_kernel, n_level=n_level, quarter=quarter, per_pixel=per_pixel),
        out_shape=pltpu.VMEM((n_level, 1, 2 * quarter), F32),
        scratch_shapes=[pltpu.VMEM((n_level, quarter * per_pixel), F32)] * 2,
        name="blend",
    )(back, owner, ranks)
    slabs = lax.all_to_all(slab, "level", split_axis=0, concat_axis=0, tiled=True)
    slabs = pltpu.with_memory_space_constraint(slabs, pltpu.VMEM)
    image_color, transmittance = pl.pallas_call(
        finish_kernel,
        out_shape=(jax.ShapeDtypeStruct((1, quarter), F32),) * 2,
        name="finish",
    )(slabs)
    return (image_color.reshape(quarter), transmittance.reshape(quarter))


def solution(mesh):
    split = P(AXES)
    rows = P(AXES, None)
    return jax.shard_map(
        shards,
        mesh=mesh,
        in_specs=(P("morton", None), P("morton", None), rows, rows)
        + (split,) * 4
        + (rows,)
        + (split,) * 4,
        out_specs=(split, split),
        check_vma=False,
    )
```
